32 devices in a mesh: af: 16 (over z, y, x), sa: 2 (over core).
Axes of the slice: x: 2, y: 2, z: 4, core: 2. Of those that a mesh axis runs over, the one named last changes fastest.
Arguments:
- series: float32 [8, 262144], P('sa', 'af'), parts along dimension 0, may hold values from -48 to 48
- tapers: float32 [10, 262144], P(None, 'af'), may hold values from -16 to 16
- concentration: float32 [10], replicated, may hold values from 0.2 to 0.95
- qi_weights: float32 [4, 10, 10], replicated, may hold values from -0.625 to 0.625
Outputs:
- spectrum: float32 [8, 16, 16384], P('sa', 'af'), parts along dimension 0
- qi_terms: float32 [8, 4, 16, 16384], P('sa', None, 'af'), parts along dimension 0
The draws below stay inside these ranges and needn't reach their ends.
There are 2 independent parts, one for each index of `sa`. The reference program is written for one: setup_inputs(seed, part) draws one part's arguments, and reference() takes and returns one part's arrays. A program takes and returns all parts, laid end to end along the dimension named above; an argument that names none is the same for every part. Nothing has to cross between parts.
All inputs are finite; a program needn't handle non-finite values.
Results may differ from the reference program's by a relative error of at most 0.0001.
Values sent between devices are 32-bit elements; how exact they have to be, the bound alone decides.
A program may use at most 128 MiB of HBM per device.

```python
import math
import jax
import jax.numpy as jnp
from jax import lax

K = 10
L = 4
ITERS = 3
SERIES = 4
TIME_DEV = 16384
SAMPLES = 262144
N_AF = 16


def draw_series(key, part):
    noise_key = jax.random.fold_in(key, 17)
    cycle_key = jax.random.fold_in(key, 29)
    time_frac = jnp.arange(SAMPLES, dtype=jnp.float32) / SAMPLES
    period = SAMPLES // TIME_DEV
    noise_part = jnp.clip(jax.random.normal(noise_key, (SERIES, SAMPLES), jnp.float32), -6.0, 6.0)
    memory_coef = 0.9
    envelope = jnp.exp(math.log(3.0) * time_frac)
    cycle_part = jnp.clip(jax.random.normal(cycle_key, (SERIES, TIME_DEV), jnp.float32), -4.0, 4.0)
    strength = 3.0
    shifted = jnp.roll(noise_part, 1, axis=1)
    repeated = jnp.tile(cycle_part, (1, period))
    return ((noise_part + memory_coef * shifted) * envelope[None, :] + strength * repeated).astype(jnp.float32)


def draw_tapers(key, part):
    coef_key = jax.random.fold_in(key, 41)
    rough_key = jax.random.fold_in(key, 43)
    harmonic_count = K + 2
    positions = (jnp.arange(SAMPLES, dtype=jnp.float32) + 1.0) / (SAMPLES + 1)
    harmonics = jnp.arange(1, harmonic_count + 1, dtype=jnp.float32)
    sine_basis = jnp.sin(math.pi * harmonics[:, None] * positions[None, :])
    coeffs = jnp.clip(jax.random.normal(coef_key, (K, harmonic_count), jnp.float32), -3.0, 3.0) * math.sqrt(2.0 / harmonic_count)
    rough_part = jnp.clip(jax.random.normal(rough_key, (K, SAMPLES), jnp.float32), -4.0, 4.0) * 0.15
    smooth = jnp.dot(coeffs, sine_basis, precision=lax.Precision.HIGHEST)
    return (smooth + rough_part).astype(jnp.float32)


def noise(own_key, extent, width, reach, kind=jnp.bfloat16):
    return jnp.clip(width * jax.random.normal(own_key, extent, jnp.float32), -reach, reach).astype(kind)


def setup_inputs(seed: int = 0, part: int = 0) -> dict:
    keys = jax.random.split(jax.random.key(seed), 5)
    part_keys = jax.random.split(jax.random.fold_in(keys[4], part), 5)
    return {
        "series": draw_series(jax.random.fold_in(jax.random.fold_in(keys[4], part), 71), part),
        "tapers": draw_tapers(jax.random.fold_in(keys[4], 71), part),
        "concentration": jnp.clip(jax.random.uniform(keys[2], (K,), jnp.float32, 0.2, 0.95), 0.2, 0.95),
        "qi_weights": noise(keys[3], (L, K, K), (K * K) ** -0.5, 0.625, jnp.float32),
    }


def reference(series, tapers, concentration, qi_weights):
    highest = lax.Precision.HIGHEST
    retained = concentration[:, None]
    unit_scale = 1.0 / math.sqrt(SAMPLES)
    spectra = []
    term_list = []
    for series_index in range(SERIES):
        scaled = series[series_index] * unit_scale
        coeffs = jnp.fft.fft(tapers * scaled[None, :], axis=1)
        coeffs = coeffs.reshape(K, TIME_DEV, N_AF).transpose(0, 2, 1).reshape(K, SAMPLES)
        real_part = jnp.real(coeffs)
        imag_part = jnp.imag(coeffs)
        powers = real_part * real_part + imag_part * imag_part
        per_term = []
        for term_index in range(L):
            mixed_re = jnp.dot(qi_weights[term_index], real_part, precision=highest)
            mixed_im = jnp.dot(qi_weights[term_index], imag_part, precision=highest)
            per_term.append(lax.optimization_barrier(jnp.sum(real_part * mixed_re + imag_part * mixed_im, axis=0)))
        estimate = 0.5 * (powers[0] + powers[1])
        for sweep_index in range(ITERS):
            variance = jnp.mean(estimate)
            weight = retained / (retained * estimate[None, :] + (1.0 - retained) * variance) ** 2
            estimate = lax.optimization_barrier(jnp.sum(weight * powers, axis=0)) / lax.optimization_barrier(jnp.sum(weight, axis=0))
        spectra.append(estimate.reshape(N_AF, TIME_DEV))
        term_list.append(jnp.stack(per_term).reshape(L, N_AF, TIME_DEV))
    return (jnp.stack(spectra), jnp.stack(term_list))
```

```python
import functools
import math

import jax
import jax.numpy as jnp
import numpy as np
from jax import lax
from jax.experimental import pallas as pl
from jax.experimental.pallas import tpu as pltpu
from jax.sharding import PartitionSpec as P

ITERS = 3
LANES = 128
CHUNK = 16


def add(a, b):
    if a is None:
        return b
    return a if b is None else a + b


def sub(a, b):
    if b is None:
        return a
    return -b if a is None else a - b


def butterfly(values):
    n = len(values)
    if n == 1:
        return values
    even, odd = butterfly(values[0::2]), butterfly(values[1::2])
    low, high = [], []
    for k in range(n // 2):
        (er, ei), (tr, ti) = even[k], odd[k]
        if 4 * k == n:
            tr, ti = ti, (None if tr is None else -tr)
        elif k:
            c, s = math.cos(2 * math.pi * k / n), math.sin(2 * math.pi * k / n)
            if ti is None:
                tr, ti = tr * c, tr * (-s)
            else:
                tr, ti = tr * c + ti * s, ti * c - tr * s
        low.append((add(er, tr), add(ei, ti)))
        high.append((sub(er, tr), sub(ei, ti)))
    return low + high


def front_kernel(series_ref, tapers_ref, twist_ref, out_ref):
    shards, tapers = tapers_ref.shape[0], tapers_ref.shape[1]

    def body(k, carry):
        got = [(series_ref[p, 0] * tapers_ref[p, k], None) for p in range(shards)]
        for q, (re, im) in enumerate(butterfly(got)):
            c, s = twist_ref[0, q], twist_ref[1, q]
            if im is None:
                out_ref[q, 0, 0, k], out_ref[q, 1, 0, k] = re * c, re * (-s)
            else:
                out_ref[q, 0, 0, k] = re * c + im * s
                out_ref[q, 1, 0, k] = im * c - re * s
        return carry

    lax.fori_loop(0, tapers, body, 0)


def split(x):
    high = x.astype(jnp.bfloat16)
    return high, (x - high.astype(jnp.float32)).astype(jnp.bfloat16)


def dot3(a, b):
    dot = functools.partial(jnp.dot, preferred_element_type=jnp.float32)
    return dot(a[0], b[0]) + (dot(a[0], b[1]) + dot(a[1], b[0]))


def refine(estimate, powers, keep, variance):
    top = bottom = None
    for k, power in enumerate(powers):
        base = keep[k] * estimate + (1.0 - keep[k]) * variance
        weight = keep[k] / (base * base)
        top = add(top, weight * power)
        bottom = add(bottom, weight)
    return top / bottom


def back_kernel(keep_ref, pair_ref, var_ref, recv_ref, left_ref, right_ref, inner_ref,
                power_ref, est_ref, qi_ref, spec, qi):
    tapers = recv_ref.shape[3]
    rows = spec.shape[2]
    terms = qi.shape[0]
    left = (left_ref[0], left_ref[1])
    right = (right_ref[0], right_ref[1])

    def transform(k, carry):
        re = recv_ref[:, 0, 0, k].reshape(rows, LANES)
        im = recv_ref[:, 1, 0, k].reshape(rows, LANES)
        mid = dot3(left, split(jnp.concatenate([re, im], axis=0)))
        mr, mi = mid[:rows], mid[rows:]
        c, s = inner_ref[0], inner_ref[1]
        turned = jnp.concatenate([mr * c + mi * s, mi * c - mr * s], axis=1)
        done = dot3(split(turned), right)
        spec[0, k] = done[:, :LANES]
        spec[1, k] = done[:, LANES:]
        return carry

    lax.fori_loop(0, tapers, transform, 0)
    variance = var_ref[pl.program_id(0)]
    keep = [keep_ref[k] for k in range(tapers)]

    def combine(i, carry):
        at = pl.ds(pl.multiple_of(i * CHUNK, CHUNK), CHUNK)
        re = [spec[0, k, at] for k in range(tapers)]
        im = [spec[1, k, at] for k in range(tapers)]
        sums = [None] * terms
        powers = []
        pair = 0
        for j in range(tapers):
            for k in range(j, tapers):
                both = re[j] * re[k] + im[j] * im[k]
                if j == k:
                    powers.append(both)
                    power_ref[0, j, at] = both
                for t in range(terms):
                    sums[t] = add(sums[t], pair_ref[t, pair] * both)
                pair += 1
        for t in range(terms):
            qi[t, at] = sums[t]
        est_ref[0, at] = refine(0.5 * (powers[0] + powers[1]), powers, keep, variance)
        return carry

    lax.fori_loop(0, rows // CHUNK, combine, 0)
    for t in range(terms):
        qi_ref[0, t] = qi[t].T


def sweep_kernel(last, keep_ref, var_ref, power_ref, est_ref, out_ref, hold):
    tapers, rows = power_ref.shape[1], power_ref.shape[2]
    variance = var_ref[pl.program_id(0)]
    keep = [keep_ref[k] for k in range(tapers)]

    def body(i, carry):
        at = pl.ds(pl.multiple_of(i * CHUNK, CHUNK), CHUNK)
        powers = [power_ref[0, k, at] for k in range(tapers)]
        hold[at] = refine(est_ref[0, at], powers, keep, variance)
        return carry

    lax.fori_loop(0, rows // CHUNK, body, 0)
    out_ref[0] = hold[...].T if last else hold[...]


def whole(shape):
    return pl.BlockSpec(shape, lambda i: (0,) * len(shape))


def each(shape, axis):
    return pl.BlockSpec(shape, lambda i: tuple(i if d == axis else 0 for d in range(len(shape))))


def smem():
    return pl.BlockSpec(memory_space=pltpu.SMEM)


def complex_table(n, left):
    angle = 2 * np.pi * (np.outer(np.arange(n), np.arange(n)) % n) / n
    c, s = np.cos(angle), np.sin(angle)
    full = np.block([[c, s], [-s, c]])
    full = jnp.asarray((full if left else full.T).astype(np.float32))
    return jnp.stack(split(full))


def phase(a, b, modulus):
    angles = (a * b % modulus).astype(jnp.float32) * (2.0 * math.pi / modulus)
    return jnp.stack([jnp.cos(angles), jnp.sin(angles)])


def local(series, tapers, concentration, qi_weights):
    shards = lax.axis_size("af")
    rank = lax.axis_index("af")
    count, local_len = series.shape
    taper_count = tapers.shape[0]
    terms = qi_weights.shape[0]
    block_len = local_len // shards
    sub_rows = block_len // LANES
    rows = local_len // LANES
    length_all = local_len * shards
    f32 = jnp.float32

    both = jnp.concatenate([series * (1.0 / math.sqrt(length_all)), tapers], axis=0)
    both = both.reshape(count + taper_count, shards, sub_rows, LANES).transpose(1, 0, 2, 3)
    got = lax.all_to_all(both, "af", split_axis=0, concat_axis=0, tiled=True)
    got_series, got_tapers = got[:, :count], got[:, count:]

    first = jnp.sum((got_series * got_tapers[:, :1]) ** 2, axis=(0, 2, 3))
    second = jnp.sum((got_series * got_tapers[:, 1:2]) ** 2, axis=(0, 2, 3))
    variance = lax.psum(0.5 * (first + second), "af")

    pos = rank * block_len + jnp.arange(block_len, dtype=jnp.int32)
    twist = phase(jnp.arange(shards, dtype=jnp.int32)[:, None], pos[None, :], length_all)
    twist = twist.reshape(2, shards, sub_rows, LANES)
    turned = pl.pallas_call(
        front_kernel,
        grid=(count,),
        out_shape=jax.ShapeDtypeStruct((shards, 2, count, taper_count, sub_rows, LANES), f32),
        in_specs=[
            each((shards, 1, sub_rows, LANES), 1),
            whole((shards, taper_count, sub_rows, LANES)),
            whole((2, shards, sub_rows, LANES)),
        ],
        out_specs=each((shards, 2, 1, taper_count, sub_rows, LANES), 2),
    )(got_series, got_tapers, twist)
    recv = lax.all_to_all(turned, "af", split_axis=0, concat_axis=0, tiled=True)

    inner = phase(
        jnp.arange(rows, dtype=jnp.int32)[:, None],
        jnp.arange(LANES, dtype=jnp.int32)[None, :],
        local_len,
    )
    symmetric = qi_weights + qi_weights.transpose(0, 2, 1)
    pairs = jnp.stack(
        [
            qi_weights[:, j, j] if j == k else symmetric[:, j, k]
            for j in range(taper_count)
            for k in range(j, taper_count)
        ],
        axis=1,
    )
    plane = (1, rows, LANES)
    flat = (1, LANES, rows)
    powers, estimate, qi_terms = pl.pallas_call(
        back_kernel,
        grid=(count,),
        out_shape=(
            jax.ShapeDtypeStruct((count, taper_count, rows, LANES), f32),
            jax.ShapeDtypeStruct((count, rows, LANES), f32),
            jax.ShapeDtypeStruct((count, terms, LANES, rows), f32),
        ),
        in_specs=[
            smem(),
            smem(),
            smem(),
            each((shards, 2, 1, taper_count, sub_rows, LANES), 2),
            whole((2, 2 * rows, 2 * rows)),
            whole((2, 2 * LANES, 2 * LANES)),
            whole((2, rows, LANES)),
        ],
        out_specs=(
            each((1, taper_count, rows, LANES), 0),
            each(plane, 0),
            each((1, terms, LANES, rows), 0),
        ),
        scratch_shapes=[
            pltpu.VMEM((2, taper_count, rows, LANES), f32),
            pltpu.VMEM((terms, rows, LANES), f32),
        ],
    )(
        concentration, pairs, variance, recv, complex_table(rows, True), complex_table(LANES, False), inner
    )
    for sweep in range(1, ITERS):
        variance = lax.psum(jnp.sum(estimate, axis=(1, 2)), "af") / length_all
        last = sweep == ITERS - 1
        shape = flat if last else plane
        estimate = pl.pallas_call(
            functools.partial(sweep_kernel, last),
            grid=(count,),
            out_shape=jax.ShapeDtypeStruct((count,) + shape[1:], f32),
            in_specs=[smem(), smem(), each((1, taper_count, rows, LANES), 0), each(plane, 0)],
            out_specs=each(shape, 0),
            scratch_shapes=[pltpu.VMEM((rows, LANES), f32)],
        )(concentration, variance, powers, estimate)
    return (
        estimate.reshape(count, 1, local_len),
        qi_terms.reshape(count, terms, 1, local_len),
    )


def solution(mesh):
    placed = (P("sa", "af"), P(None, "af"), P(), P())
    return jax.shard_map(
        local,
        mesh=mesh,
        in_specs=placed,
        out_specs=(P("sa", "af", None), P("sa", None, "af", None)),
        check_vma=False,
    )
```

```python
import functools
import math

import jax
import jax.numpy as jnp
import numpy as np
from jax import lax
from jax.experimental import pallas as pl
from jax.experimental.pallas import tpu as pltpu
from jax.sharding import PartitionSpec as P

ITERS = 3
LANES = 128
CHUNK = 16


def add(a, b):
    if a is None:
        return b
    return a if b is None else a + b


def sub(a, b):
    if b is None:
        return a
    return -b if a is None else a - b


def butterfly(values):
    n = len(values)
    if n == 1:
        return values
    even, odd = butterfly(values[0::2]), butterfly(values[1::2])
    low, high = [], []
    for k in range(n // 2):
        (er, ei), (tr, ti) = even[k], odd[k]
        if 4 * k == n:
            tr, ti = ti, (None if tr is None else -tr)
        elif k:
            c, s = math.cos(2 * math.pi * k / n), math.sin(2 * math.pi * k / n)
            if ti is None:
                tr, ti = tr * c, tr * (-s)
            else:
                tr, ti = tr * c + ti * s, ti * c - tr * s
        low.append((add(er, tr), add(ei, ti)))
        high.append((sub(er, tr), sub(ei, ti)))
    return low + high


def front_kernel(series_ref, tapers_ref, twist_ref, out_ref):
    shards, tapers = tapers_ref.shape[0], tapers_ref.shape[1]

    def body(k, carry):
        got = [(series_ref[p, 0] * tapers_ref[p, k], None) for p in range(shards)]
        for q, (re, im) in enumerate(butterfly(got)):
            c, s = twist_ref[0, q], twist_ref[1, q]
            if im is None:
                out_ref[q, 0, 0, k], out_ref[q, 1, 0, k] = re * c, re * (-s)
            else:
                out_ref[q, 0, 0, k] = re * c + im * s
                out_ref[q, 1, 0, k] = im * c - re * s
        return carry

    lax.fori_loop(0, tapers, body, 0)


def split(x):
    high = x.astype(jnp.bfloat16)
    return high, (x - high.astype(jnp.float32)).astype(jnp.bfloat16)


def dot3(a, b):
    dot = functools.partial(jnp.dot, preferred_element_type=jnp.float32)
    return dot(a[0], b[0]) + (dot(a[0], b[1]) + dot(a[1], b[0]))


def refine(estimate, powers, keep, variance):
    top = bottom = None
    for k, power in enumerate(powers):
        base = keep[k] * estimate + (1.0 - keep[k]) * variance
        weight = keep[k] / (base * base)
        top = add(top, weight * power)
        bottom = add(bottom, weight)
    return top / bottom


def back_kernel(keep_ref, pair_ref, var_ref, recv_ref, left_ref, right_ref, inner_ref,
                power_ref, est_ref, qi_ref, spec, qi):
    tapers = recv_ref.shape[3]
    rows = spec.shape[2]
    terms = qi.shape[0]
    left = (left_ref[0], left_ref[1])
    right = (right_ref[0], right_ref[1])

    def transform(k, carry):
        re = recv_ref[:, 0, 0, k].reshape(rows, LANES)
        im = recv_ref[:, 1, 0, k].reshape(rows, LANES)
        mid = dot3(left, split(jnp.concatenate([re, im], axis=0)))
        mr, mi = mid[:rows], mid[rows:]
        c, s = inner_ref[0], inner_ref[1]
        turned = jnp.concatenate([mr * c + mi * s, mi * c - mr * s], axis=1)
        done = dot3(split(turned), right)
        spec[0, k] = done[:, :LANES]
        spec[1, k] = done[:, LANES:]
        return carry

    lax.fori_loop(0, tapers, transform, 0)
    variance = var_ref[pl.program_id(0)]
    keep = [keep_ref[k] for k in range(tapers)]

    def combine(i, carry):
        at = pl.ds(pl.multiple_of(i * CHUNK, CHUNK), CHUNK)
        re = [spec[0, k, at] for k in range(tapers)]
        im = [spec[1, k, at] for k in range(tapers)]
        sums = [None] * terms
        powers = []
        pair = 0
        for j in range(tapers):
            for k in range(j, tapers):
                both = re[j] * re[k] + im[j] * im[k]
                if j == k:
                    powers.append(both)
                    power_ref[0, j, at] = both
                for t in range(terms):
                    sums[t] = add(sums[t], pair_ref[t, pair] * both)
                pair += 1
        for t in range(terms):
            qi[t, at] = sums[t]
        est_ref[0, at] = refine(0.5 * (powers[0] + powers[1]), powers, keep, variance)
        return carry

    lax.fori_loop(0, rows // CHUNK, combine, 0)
    for t in range(terms):
        qi_ref[0, t] = qi[t].T


def sweep_kernel(last, keep_ref, var_ref, power_ref, est_ref, out_ref, hold):
    tapers, rows = power_ref.shape[1], power_ref.shape[2]
    variance = var_ref[pl.program_id(0)]
    keep = [keep_ref[k] for k in range(tapers)]

    def body(i, carry):
        at = pl.ds(pl.multiple_of(i * CHUNK, CHUNK), CHUNK)
        powers = [power_ref[0, k, at] for k in range(tapers)]
        hold[at] = refine(est_ref[0, at], powers, keep, variance)
        return carry

    lax.fori_loop(0, rows // CHUNK, body, 0)
    out_ref[0] = hold[...].T if last else hold[...]


def whole(shape):
    return pl.BlockSpec(shape, lambda i: (0,) * len(shape))


def each(shape, axis):
    return pl.BlockSpec(shape, lambda i: tuple(i if d == axis else 0 for d in range(len(shape))))


def smem():
    return pl.BlockSpec(memory_space=pltpu.SMEM)


def complex_table(n, left):
    angle = 2 * np.pi * (np.outer(np.arange(n), np.arange(n)) % n) / n
    c, s = np.cos(angle), np.sin(angle)
    full = np.block([[c, s], [-s, c]])
    full = jnp.asarray((full if left else full.T).astype(np.float32))
    return jnp.stack(split(full))


def phase(a, b, modulus):
    angles = (a * b % modulus).astype(jnp.float32) * (2.0 * math.pi / modulus)
    return jnp.stack([jnp.cos(angles), jnp.sin(angles)])


def local(series, tapers, concentration, qi_weights):
    shards = lax.axis_size("af")
    rank = lax.axis_index("af")
    count, local_len = series.shape
    taper_count = tapers.shape[0]
    terms = qi_weights.shape[0]
    block_len = local_len // shards
    sub_rows = block_len // LANES
    rows = local_len // LANES
    length_all = local_len * shards
    f32 = jnp.float32

    scaled = series * (1.0 / math.sqrt(length_all))
    energy = 0.5 * jnp.sum((scaled * tapers[:1]) ** 2 + (scaled * tapers[1:2]) ** 2, axis=1)
    energy_row = jnp.tile(jnp.pad(energy, (0, LANES - count)), rows)[None]
    both = jnp.concatenate([scaled, tapers, energy_row], axis=0)
    both = both.reshape(count + taper_count + 1, shards, sub_rows, LANES).transpose(1, 0, 2, 3)
    got = lax.all_to_all(both, "af", split_axis=0, concat_axis=0, tiled=True)
    got_series, got_tapers = got[:, :count], got[:, count:-1]
    variance = jnp.sum(got[:, -1, 0, :count], axis=0)

    pos = rank * block_len + jnp.arange(block_len, dtype=jnp.int32)
    twist = phase(jnp.arange(shards, dtype=jnp.int32)[:, None], pos[None, :], length_all)
    twist = twist.reshape(2, shards, sub_rows, LANES)
    turned = pl.pallas_call(
        front_kernel,
        grid=(count,),
        out_shape=jax.ShapeDtypeStruct((shards, 2, count, taper_count, sub_rows, LANES), f32),
        in_specs=[
            each((shards, 1, sub_rows, LANES), 1),
            whole((shards, taper_count, sub_rows, LANES)),
            whole((2, shards, sub_rows, LANES)),
        ],
        out_specs=each((shards, 2, 1, taper_count, sub_rows, LANES), 2),
    )(got_series, got_tapers, twist)
    recv = lax.all_to_all(turned, "af", split_axis=0, concat_axis=0, tiled=True)

    inner = phase(
        jnp.arange(rows, dtype=jnp.int32)[:, None],
        jnp.arange(LANES, dtype=jnp.int32)[None, :],
        local_len,
    )
    symmetric = qi_weights + qi_weights.transpose(0, 2, 1)
    pairs = jnp.stack(
        [
            qi_weights[:, j, j] if j == k else symmetric[:, j, k]
            for j in range(taper_count)
            for k in range(j, taper_count)
        ],
        axis=1,
    )
    plane = (1, rows, LANES)
    flat = (1, LANES, rows)
    powers, estimate, qi_terms = pl.pallas_call(
        back_kernel,
        grid=(count,),
        out_shape=(
            jax.ShapeDtypeStruct((count, taper_count, rows, LANES), f32),
            jax.ShapeDtypeStruct((count, rows, LANES), f32),
            jax.ShapeDtypeStruct((count, terms, LANES, rows), f32),
        ),
        in_specs=[
            smem(),
            smem(),
            smem(),
            each((shards, 2, 1, taper_count, sub_rows, LANES), 2),
            whole((2, 2 * rows, 2 * rows)),
            whole((2, 2 * LANES, 2 * LANES)),
            whole((2, rows, LANES)),
        ],
        out_specs=(
            each((1, taper_count, rows, LANES), 0),
            each(plane, 0),
            each((1, terms, LANES, rows), 0),
        ),
        scratch_shapes=[
            pltpu.VMEM((2, taper_count, rows, LANES), f32),
            pltpu.VMEM((terms, rows, LANES), f32),
        ],
    )(
        concentration, pairs, variance, recv, complex_table(rows, True), complex_table(LANES, False), inner
    )
    for sweep in range(1, ITERS):
        sums = lax.all_gather(jnp.sum(estimate, axis=(1, 2)), "af")
        variance = jnp.sum(sums, axis=0) / length_all
        last = sweep == ITERS - 1
        shape = flat if last else plane
        estimate = pl.pallas_call(
            functools.partial(sweep_kernel, last),
            grid=(count,),
            out_shape=jax.ShapeDtypeStruct((count,) + shape[1:], f32),
            in_specs=[smem(), smem(), each((1, taper_count, rows, LANES), 0), each(plane, 0)],
            out_specs=each(shape, 0),
            scratch_shapes=[pltpu.VMEM((rows, LANES), f32)],
        )(concentration, variance, powers, estimate)
    return (
        estimate.reshape(count, 1, local_len),
        qi_terms.reshape(count, terms, 1, local_len),
    )


def solution(mesh):
    placed = (P("sa", "af"), P(None, "af"), P(), P())
    return jax.shard_map(
        local,
        mesh=mesh,
        in_specs=placed,
        out_specs=(P("sa", "af", None), P("sa", None, "af", None)),
        check_vma=False,
    )
```

```python
import functools
import math

import jax
import jax.numpy as jnp
import numpy as np
from jax import lax
from jax.experimental import pallas as pl
from jax.experimental.pallas import tpu as pltpu
from jax.sharding import PartitionSpec as P

ITERS = 3
LANES = 128
CHUNK = 16


def add(a, b):
    if a is None:
        return b
    return a if b is None else a + b


def sub(a, b):
    if b is None:
        return a
    return -b if a is None else a - b


def butterfly(values):
    n = len(values)
    if n == 1:
        return values
    even, odd = butterfly(values[0::2]), butterfly(values[1::2])
    low, high = [], []
    for k in range(n // 2):
        (er, ei), (tr, ti) = even[k], odd[k]
        if 4 * k == n:
            tr, ti = ti, (None if tr is None else -tr)
        elif k:
            c, s = math.cos(2 * math.pi * k / n), math.sin(2 * math.pi * k / n)
            if ti is None:
                tr, ti = tr * c, tr * (-s)
            else:
                tr, ti = tr * c + ti * s, ti * c - tr * s
        low.append((add(er, tr), add(ei, ti)))
        high.append((sub(er, tr), sub(ei, ti)))
    return low + high


def front_kernel(series_ref, tapers_ref, twist_ref, out_ref):
    shards, tapers = tapers_ref.shape[0], tapers_ref.shape[1]

    def body(k, carry):
        got = [(series_ref[p, 0] * tapers_ref[p, k], None) for p in range(shards)]
        for q, (re, im) in enumerate(butterfly(got)):
            c, s = twist_ref[0, q], twist_ref[1, q]
            if im is None:
                out_ref[q, 0, 0, k], out_ref[q, 1, 0, k] = re * c, re * (-s)
            else:
                out_ref[q, 0, 0, k] = re * c + im * s
                out_ref[q, 1, 0, k] = im * c - re * s
        return carry

    lax.fori_loop(0, tapers, body, 0)


def split(x):
    high = x.astype(jnp.bfloat16)
    return high, (x - high.astype(jnp.float32)).astype(jnp.bfloat16)


def dot3(a, b):
    dot = functools.partial(jnp.dot, preferred_element_type=jnp.float32)
    return dot(a[0], b[0]) + (dot(a[0], b[1]) + dot(a[1], b[0]))


def refine(estimate, powers, keep, variance):
    top = bottom = None
    for k, power in enumerate(powers):
        base = keep[k] * estimate + (1.0 - keep[k]) * variance
        weight = keep[k] / (base * base)
        top = add(top, weight * power)
        bottom = add(bottom, weight)
    return top / bottom


def back_kernel(keep_ref, pair_ref, var_ref, recv_ref, left_ref, right_ref, inner_ref,
                power_ref, est_ref, qi_ref, spec, qi):
    tapers = recv_ref.shape[3]
    rows = spec.shape[2]
    terms = qi.shape[0]
    left = (left_ref[0], left_ref[1])
    right = (right_ref[0], right_ref[1])

    def transform(k, carry):
        re = recv_ref[:, 0, 0, k].reshape(rows, LANES)
        im = recv_ref[:, 1, 0, k].reshape(rows, LANES)
        mid = dot3(left, split(jnp.concatenate([re, im], axis=0)))
        mr, mi = mid[:rows], mid[rows:]
        c, s = inner_ref[0], inner_ref[1]
        turned = jnp.concatenate([mr * c + mi * s, mi * c - mr * s], axis=1)
        done = dot3(split(turned), right)
        spec[0, k] = done[:, :LANES]
        spec[1, k] = done[:, LANES:]
        return carry

    lax.fori_loop(0, tapers, transform, 0)
    variance = var_ref[pl.program_id(0)]
    keep = [keep_ref[k] for k in range(tapers)]

    def combine(i, carry):
        at = pl.ds(pl.multiple_of(i * CHUNK, CHUNK), CHUNK)
        re = [spec[0, k, at] for k in range(tapers)]
        im = [spec[1, k, at] for k in range(tapers)]
        sums = [None] * terms
        powers = []
        pair = 0
        for j in range(tapers):
            for k in range(j, tapers):
                both = re[j] * re[k] + im[j] * im[k]
                if j == k:
                    powers.append(both)
                    power_ref[0, j, at] = both
                for t in range(terms):
                    sums[t] = add(sums[t], pair_ref[t, pair] * both)
                pair += 1
        for t in range(terms):
            qi[t, at] = sums[t]
        est_ref[0, at] = refine(0.5 * (powers[0] + powers[1]), powers, keep, variance)
        return carry

    lax.fori_loop(0, rows // CHUNK, combine, 0)
    for t in range(terms):
        qi_ref[0, t] = qi[t].T


def sweep_kernel(last, keep_ref, var_ref, power_ref, est_ref, out_ref, hold):
    tapers, rows = power_ref.shape[1], power_ref.shape[2]
    variance = var_ref[pl.program_id(0)]
    keep = [keep_ref[k] for k in range(tapers)]

    def body(i, carry):
        at = pl.ds(pl.multiple_of(i * CHUNK, CHUNK), CHUNK)
        powers = [power_ref[0, k, at] for k in range(tapers)]
        hold[at] = refine(est_ref[0, at], powers, keep, variance)
        return carry

    lax.fori_loop(0, rows // CHUNK, body, 0)
    out_ref[0] = hold[...].T if last else hold[...]


def total_kernel(part_ref, out_ref, slots, send_sem, recv_sem):
    shards = slots.shape[0]
    me = lax.axis_index("af")
    barrier = pltpu.get_barrier_semaphore()
    peers = [lax.rem(me + d, shards) for d in range(shards)]
    for peer in peers[1:]:
        pl.semaphore_signal(
            barrier, inc=1, device_id={"af": peer}, device_id_type=pl.DeviceIdType.MESH
        )
    pl.semaphore_wait(barrier, shards - 1)
    copies = []
    for d in range(1, shards):
        copy = pltpu.make_async_remote_copy(
            src_ref=part_ref,
            dst_ref=slots.at[d],
            send_sem=send_sem.at[d],
            recv_sem=recv_sem.at[d],
            device_id={"af": peers[d]},
            device_id_type=pl.DeviceIdType.MESH,
        )
        copy.start()
        copies.append(copy)
    total = part_ref[...]
    for d, copy in enumerate(copies, 1):
        copy.wait()
        total += slots[d]
    out_ref[...] = total


def total_over_devices(part, shards, ident):
    vmem = pl.BlockSpec(memory_space=pltpu.VMEM)
    return pl.pallas_call(
        total_kernel,
        out_shape=jax.ShapeDtypeStruct(part.shape, part.dtype),
        in_specs=[vmem],
        out_specs=vmem,
        scratch_shapes=[
            pltpu.VMEM((shards,) + part.shape, part.dtype),
            pltpu.SemaphoreType.DMA((shards,)),
            pltpu.SemaphoreType.DMA((shards,)),
        ],
        compiler_params=pltpu.CompilerParams(collective_id=ident, has_side_effects=True),
    )(part)


def whole(shape):
    return pl.BlockSpec(shape, lambda i: (0,) * len(shape))


def each(shape, axis):
    return pl.BlockSpec(shape, lambda i: tuple(i if d == axis else 0 for d in range(len(shape))))


def smem():
    return pl.BlockSpec(memory_space=pltpu.SMEM)


def complex_table(n, left):
    angle = 2 * np.pi * (np.outer(np.arange(n), np.arange(n)) % n) / n
    c, s = np.cos(angle), np.sin(angle)
    full = np.block([[c, s], [-s, c]])
    full = jnp.asarray((full if left else full.T).astype(np.float32))
    return jnp.stack(split(full))


def phase(a, b, modulus):
    angles = (a * b % modulus).astype(jnp.float32) * (2.0 * math.pi / modulus)
    return jnp.stack([jnp.cos(angles), jnp.sin(angles)])


def local(series, tapers, concentration, qi_weights):
    shards = lax.axis_size("af")
    rank = lax.axis_index("af")
    count, local_len = series.shape
    taper_count = tapers.shape[0]
    terms = qi_weights.shape[0]
    block_len = local_len // shards
    sub_rows = block_len // LANES
    rows = local_len // LANES
    length_all = local_len * shards
    f32 = jnp.float32

    scaled = series * (1.0 / math.sqrt(length_all))
    energy = 0.5 * jnp.sum((scaled * tapers[:1]) ** 2 + (scaled * tapers[1:2]) ** 2, axis=1)
    energy_row = jnp.tile(jnp.pad(energy, (0, LANES - count)), rows)[None]
    both = jnp.concatenate([scaled, tapers, energy_row], axis=0)
    both = both.reshape(count + taper_count + 1, shards, sub_rows, LANES).transpose(1, 0, 2, 3)
    got = lax.all_to_all(both, "af", split_axis=0, concat_axis=0, tiled=True)
    got_series, got_tapers = got[:, :count], got[:, count:-1]
    variance = jnp.sum(got[:, -1, 0, :count], axis=0)

    pos = rank * block_len + jnp.arange(block_len, dtype=jnp.int32)
    twist = phase(jnp.arange(shards, dtype=jnp.int32)[:, None], pos[None, :], length_all)
    twist = twist.reshape(2, shards, sub_rows, LANES)
    turned = pl.pallas_call(
        front_kernel,
        grid=(count,),
        out_shape=jax.ShapeDtypeStruct((shards, 2, count, taper_count, sub_rows, LANES), f32),
        in_specs=[
            each((shards, 1, sub_rows, LANES), 1),
            whole((shards, taper_count, sub_rows, LANES)),
            whole((2, shards, sub_rows, LANES)),
        ],
        out_specs=each((shards, 2, 1, taper_count, sub_rows, LANES), 2),
    )(got_series, got_tapers, twist)
    recv = lax.all_to_all(turned, "af", split_axis=0, concat_axis=0, tiled=True)

    inner = phase(
        jnp.arange(rows, dtype=jnp.int32)[:, None],
        jnp.arange(LANES, dtype=jnp.int32)[None, :],
        local_len,
    )
    symmetric = qi_weights + qi_weights.transpose(0, 2, 1)
    pairs = jnp.stack(
        [
            qi_weights[:, j, j] if j == k else symmetric[:, j, k]
            for j in range(taper_count)
            for k in range(j, taper_count)
        ],
        axis=1,
    )
    plane = (1, rows, LANES)
    flat = (1, LANES, rows)
    powers, estimate, qi_terms = pl.pallas_call(
        back_kernel,
        grid=(count,),
        out_shape=(
            jax.ShapeDtypeStruct((count, taper_count, rows, LANES), f32),
            jax.ShapeDtypeStruct((count, rows, LANES), f32),
            jax.ShapeDtypeStruct((count, terms, LANES, rows), f32),
        ),
        in_specs=[
            smem(),
            smem(),
            smem(),
            each((shards, 2, 1, taper_count, sub_rows, LANES), 2),
            whole((2, 2 * rows, 2 * rows)),
            whole((2, 2 * LANES, 2 * LANES)),
            whole((2, rows, LANES)),
        ],
        out_specs=(
            each((1, taper_count, rows, LANES), 0),
            each(plane, 0),
            each((1, terms, LANES, rows), 0),
        ),
        scratch_shapes=[
            pltpu.VMEM((2, taper_count, rows, LANES), f32),
            pltpu.VMEM((terms, rows, LANES), f32),
        ],
    )(
        concentration, pairs, variance, recv, complex_table(rows, True), complex_table(LANES, False), inner
    )
    for sweep in range(1, ITERS):
        sums = total_over_devices(jnp.sum(estimate, axis=1), shards, sweep)
        variance = jnp.sum(sums, axis=1) / length_all
        last = sweep == ITERS - 1
        shape = flat if last else plane
        estimate = pl.pallas_call(
            functools.partial(sweep_kernel, last),
            grid=(count,),
            out_shape=jax.ShapeDtypeStruct((count,) + shape[1:], f32),
            in_specs=[smem(), smem(), each((1, taper_count, rows, LANES), 0), each(plane, 0)],
            out_specs=each(shape, 0),
            scratch_shapes=[pltpu.VMEM((rows, LANES), f32)],
        )(concentration, variance, powers, estimate)
    return (
        estimate.reshape(count, 1, local_len),
        qi_terms.reshape(count, terms, 1, local_len),
    )


def solution(mesh):
    placed = (P("sa", "af"), P(None, "af"), P(), P())
    return jax.shard_map(
        local,
        mesh=mesh,
        in_specs=placed,
        out_specs=(P("sa", "af", None), P("sa", None, "af", None)),
        check_vma=False,
    )
```
